32 devices in a mesh: cp: 16 (over z, x, core), tp: 2 (over y).
Axes of the slice: x: 2, y: 2, z: 4, core: 2. Of those that a mesh axis runs over, the one named last changes fastest.
Arguments:
- hidden: bfloat16 [8192, 4096], P('cp', 'tp'), may hold values from -6 to 6
- norm_gain: float32 [4096], replicated, may hold values from 0.5 to 1.5
- w_query: bfloat16 [4096, 4096], P(None, 'tp'), may hold values from -0.140625 to 0.140625
- w_key: bfloat16 [4096, 1024], P(None, 'tp'), may hold values from -4 to 4
- w_value: bfloat16 [4096, 1024], P(None, 'tp'), may hold values from -0.09375 to 0.09375
- w_out: bfloat16 [4096, 4096], P('tp'), may hold values from -0.5 to 0.5
- doc_ids: int32 [8192], P('cp'), may hold values from 0 to 5, never falling along the last dimension, each value on 1 to 6144 neighbouring positions
Outputs:
- updated: bfloat16 [8192, 4096], P('cp', 'tp')
The draws below stay inside these ranges and needn't reach their ends.
Inputs may be any that keep to these rules, and one draw needn't show every extreme that they name: `doc_ids`: document numbers never fall along the sequence; every document has 1 to 6144 tokens.
All inputs are finite; a program needn't handle non-finite values.
Results may differ from the reference program's by a relative error of at most 0.017.
The reference program's roundings to bfloat16 on the way count: a program that leaves them out, or rounds other values in their place, can miss the bound.
Values may be sent and summed in bfloat16 or wider, within the bound.
A program may use at most 128 MiB of HBM per device.

```python
import math
import jax
import jax.numpy as jnp
import numpy as np
from jax import lax

D = 4096
HEADS = 32
KV_HEADS = 8
HEAD_SIZE = 128
TOK_DEV = 512
DOCS = 6
SEQ = 8192
LONGEST = 6144
N_TP = 2


def query_key_pair(key):
    spread = 1.5 / math.sqrt(D)
    limit = 9.0 / math.sqrt(D)
    base = jax.random.normal(jax.random.fold_in(key, 101), (D, HEADS * HEAD_SIZE), jnp.float32) * spread
    base = jnp.clip(base, -limit, limit)
    other = jax.random.normal(jax.random.fold_in(key, 202), (D, KV_HEADS * HEAD_SIZE), jnp.float32) * spread
    other = jnp.clip(other, -limit, limit)
    return (base, other)


def draw_w_query(key, part):
    base, other = query_key_pair(key)
    return base.astype(jnp.bfloat16)


def draw_w_key(key, part):
    base, other = query_key_pair(key)
    result = other
    return result.astype(jnp.bfloat16)


def block_levels(rng, dims, cuts, low, top_value):
    loudness = 1.0
    for axis_at, shards_of in cuts:
        draws = jax.random.uniform(jax.random.fold_in(jax.random.fold_in(rng, 6), axis_at), (shards_of,), jnp.float32, low / len(cuts), top_value / len(cuts))
        loudness = loudness * jnp.repeat(jnp.exp(draws), dims[axis_at] // shards_of).reshape((-1,) + (1,) * (len(dims) - 1 - axis_at))
    return loudness


def length_profile(amount, total, reach, slope):
    loads = [(1 << 20) // math.isqrt(standing ** slope) + 1 for standing in range(2, amount + 1)]
    rest, given = total - reach - (amount - 1), [1] * (amount - 1)
    while rest > 0:
        free = [i for i in range(amount - 1) if given[i] < reach]
        whole, remaining = sum([loads[i] for i in free]), rest
        for i in free:
            addition = min(reach - given[i], max(1, remaining * loads[i] // whole), rest)
            given[i] = given[i] + addition
            rest = rest - addition
    return np.array([reach] + given)


def uneven(own_key, number_of, total, reach, skew):
    if number_of == 2:
        one = jax.random.randint(own_key, (), max(1, total - reach), min(reach, total - 1) + 1)
        return jnp.stack([one, total - one])
    sizes = jnp.asarray(length_profile(number_of, total, reach, skew), jnp.int32)
    twos = (number_of - 1) // 2
    donor, sink = sizes[1:1 + 2 * twos:2], sizes[2:2 + 2 * twos:2]
    slack = jnp.minimum(donor - 1, reach - sink)
    passed = jax.random.randint(jax.random.fold_in(own_key, 1), (twos,), 0, 1 << 20) % (slack + 1)
    sizes = sizes.at[1:1 + 2 * twos:2].set(donor - passed).at[2:2 + 2 * twos:2].set(sink + passed)
    return sizes[jax.random.permutation(jax.random.fold_in(own_key, 2), number_of)]


def centred(own_key, dims, scale, most, shards=(), held_as=jnp.bfloat16):
    values = scale * jax.random.normal(own_key, dims, jnp.float32)
    if shards:
        values = values * block_levels(own_key, dims, shards, -0.22, 0.18)
    return jnp.clip(values, -most, most).astype(held_as)


def setup_inputs(seed: int = 0) -> dict:
    seeds = jax.random.split(jax.random.key(seed), 8)
    return {
        "hidden": centred(seeds[0], (SEQ, D), 1.0, 6.0, ((0, 16), (1, 2))),
        "norm_gain": jnp.clip(1.0 + 0.1 * jax.random.normal(seeds[1], (D,), jnp.float32), 0.5, 1.5),
        "w_query": draw_w_query(jax.random.fold_in(seeds[7], 71), 0),
        "w_key": draw_w_key(jax.random.fold_in(seeds[7], 71), 0),
        "w_value": centred(seeds[4], (D, KV_HEADS * HEAD_SIZE), D ** -0.5, 0.09375, ((1, 2),)),
        "w_out": centred(seeds[5], (HEADS * HEAD_SIZE, D), (HEADS * HEAD_SIZE // 32) ** -0.5, 0.5, ((0, 2),)),
        "doc_ids": jnp.searchsorted(jnp.cumsum(uneven(seeds[6], DOCS, SEQ, LONGEST, 2)), jnp.arange(SEQ), side="right").astype(jnp.int32),
    }


epsilon = 1e-05
rope_base = 500000.0

def rotate(vectors, positions):
    half = HEAD_SIZE // 2
    freqs = rope_base ** (-jnp.arange(half, dtype=jnp.float32) * 2.0 / HEAD_SIZE)
    angles = positions.astype(jnp.float32)[:, None] * freqs[None, :]
    cosine = jnp.cos(angles)[:, None, :]
    sine = jnp.sin(angles)[:, None, :]
    first = vectors[..., :half]
    second = vectors[..., half:]
    return jnp.concatenate([first * cosine - second * sine, second * cosine + first * sine], axis=-1)

def attend_block(loop_state, query_matrix, query_pos, query_doc, key_matrix, value_matrix, key_pos, key_doc):
    best, total, running_output = loop_state
    logit_matrix = jnp.einsum('ucpm,ycm->cpuy', query_matrix.astype(jnp.float32), key_matrix.astype(jnp.float32)) * HEAD_SIZE ** (-0.5)
    allowed = (key_pos[None, :] <= query_pos[:, None]) & (key_doc[None, :] == query_doc[:, None])
    masked = jnp.where(allowed, logit_matrix, jnp.float32(-1e+30))
    new_best = jnp.maximum(best, lax.optimization_barrier(jnp.max(masked, axis=-1)))
    correction_scale = jnp.exp(best - new_best)
    attention_weights = jnp.where(allowed, jnp.exp(logit_matrix - new_best[..., None]), jnp.float32(0.0))
    total = total * correction_scale + lax.optimization_barrier(jnp.sum(attention_weights, axis=-1))
    rounded_weights = attention_weights.astype(jnp.bfloat16).astype(jnp.float32)
    running_output = running_output * correction_scale[..., None] + jnp.einsum('sfec,csh->sfeh', rounded_weights, value_matrix.astype(jnp.float32))
    return (new_best, total, running_output)

def reference(hidden, norm_gain, w_query, w_key, w_value, w_out, doc_ids):
    seq_len = hidden.shape[0]
    group = HEADS // KV_HEADS
    wide = hidden.astype(jnp.float32)
    inverse_rms = lax.rsqrt(lax.optimization_barrier(jnp.mean(wide * wide, axis=1, keepdims=True)) + epsilon)
    normed = (wide * inverse_rms * norm_gain.astype(jnp.float32)[None, :]).astype(jnp.bfloat16)
    positions = jnp.arange(seq_len, dtype=jnp.int32)
    query_raw = jnp.dot(normed, w_query, preferred_element_type=jnp.float32).reshape(seq_len, HEADS, HEAD_SIZE)
    key_raw = jnp.dot(normed, w_key, preferred_element_type=jnp.float32).reshape(seq_len, KV_HEADS, HEAD_SIZE)
    query_matrix = rotate(query_raw, positions).astype(jnp.bfloat16).reshape(seq_len, KV_HEADS, group, HEAD_SIZE)
    key_matrix = rotate(key_raw, positions).astype(jnp.bfloat16)
    value_matrix = jnp.dot(normed, w_value, preferred_element_type=jnp.float32).astype(jnp.bfloat16).reshape(seq_len, KV_HEADS, HEAD_SIZE)
    block_index = TOK_DEV if TOK_DEV <= 512 else 512
    blocks = seq_len // block_index

    def one_query_block(index):
        start = (index * block_index).astype(jnp.int32)
        query_blk = lax.dynamic_slice_in_dim(query_matrix, start, block_index, 0)
        query_pos = start + jnp.arange(block_index, dtype=jnp.int32)
        query_doc = lax.dynamic_slice_in_dim(doc_ids, start, block_index, 0)

        def loop_body(loop_state, key_block_index):
            key_offset = (key_block_index * block_index).astype(jnp.int32)

            def work(state):
                key_blk = lax.dynamic_slice_in_dim(key_matrix, key_offset, block_index, 0)
                value_blk = lax.dynamic_slice_in_dim(value_matrix, key_offset, block_index, 0)
                key_pos = key_offset + jnp.arange(block_index, dtype=jnp.int32)
                key_doc = lax.dynamic_slice_in_dim(doc_ids, key_offset, block_index, 0)
                return attend_block(state, query_blk, query_pos, query_doc, key_blk, value_blk, key_pos, key_doc)
            return (lax.cond(key_offset <= start + block_index - 1, work, lambda state: state, loop_state), None)
        init = (jnp.full((KV_HEADS, group, block_index), -1e+30, jnp.float32), jnp.zeros((KV_HEADS, group, block_index), jnp.float32), jnp.zeros((KV_HEADS, group, block_index, HEAD_SIZE), jnp.float32))
        final, _ = lax.scan(loop_body, init, jnp.arange(blocks, dtype=jnp.int32))
        result = final[2] / final[1][..., None]
        return jnp.transpose(result, (2, 0, 1, 3)).reshape(block_index, HEADS * HEAD_SIZE).astype(jnp.bfloat16)
    attended = lax.map(one_query_block, jnp.arange(blocks, dtype=jnp.int32)).reshape(seq_len, HEADS * HEAD_SIZE)
    width_cols = HEADS * HEAD_SIZE // N_TP
    mixed = jnp.zeros((seq_len, hidden.shape[1]), jnp.float32)
    for group_index in range(N_TP):
        lower = group_index * width_cols
        partial_sum = jnp.dot(attended[:, lower:lower + width_cols], w_out[lower:lower + width_cols], preferred_element_type=jnp.float32).astype(jnp.bfloat16)
        partial_sum = lax.optimization_barrier(partial_sum)
        mixed = mixed + partial_sum.astype(jnp.float32)
    return mixed.astype(jnp.bfloat16)
```

```python
import functools

import jax
import jax.numpy as jnp
from jax import lax
from jax.experimental import pallas as pl
from jax.experimental.pallas import tpu as pltpu
from jax.sharding import PartitionSpec as P

HEADS = 32
KV_HEADS = 8
HEAD_SIZE = 128
GROUP = HEADS // KV_HEADS

epsilon = 1e-05
rope_base = 500000.0
TILE = 256
KEYS = 512
LOG2E = 1.4426950408889634
SCALE = HEAD_SIZE ** (-0.5) * LOG2E
FLOOR = -1e29
MASKED = -1e30


def tables(positions):
    half = HEAD_SIZE // 2
    freqs = rope_base ** (-jnp.arange(half, dtype=jnp.float32) * 2.0 / HEAD_SIZE)
    angles = positions.astype(jnp.float32)[:, None] * freqs[None, :]
    cosine = jnp.cos(angles)
    sine = jnp.sin(angles)
    return (
        jnp.concatenate([cosine, cosine], axis=1),
        jnp.concatenate([-sine, sine], axis=1),
    )


def attend_kernel(
    bounds, q_ref, k_ref, v_ref, cos_ref, sin_ref, start_ref, out_ref, qs, m_ref, l_ref, acc_ref,
    *, tile0,
):
    tile = pl.program_id(1) + tile0
    lo, full_lo, full_hi, hi, first_pos = (bounds[tile, i] for i in range(5))
    for h in range(GROUP):
        raw = q_ref[:, h * HEAD_SIZE : (h + 1) * HEAD_SIZE]
        turned = raw * cos_ref[...] + pltpu.roll(raw, HEAD_SIZE // 2, 1) * sin_ref[...]
        qs[h] = turned.astype(jnp.bfloat16)
    m_ref[...] = jnp.full_like(m_ref, FLOOR)
    l_ref[...] = jnp.zeros_like(l_ref)
    acc_ref[...] = jnp.zeros_like(acc_ref)
    parts = KEYS // HEAD_SIZE

    def block(index, masking):
        rows = pl.ds(pl.multiple_of(index * KEYS, KEYS), KEYS)
        keys = k_ref[rows, :]
        values = v_ref[rows, :]
        if masking:
            row = lax.broadcasted_iota(jnp.int32, (TILE, HEAD_SIZE), 0)
            lane = lax.broadcasted_iota(jnp.int32, (TILE, HEAD_SIZE), 1)
            last = row + (first_pos - index * KEYS) - lane
            begin = start_ref[...] - index * KEYS - lane
            allowed = [
                (last >= c * HEAD_SIZE) & (begin <= c * HEAD_SIZE) for c in range(parts)
            ]
        for h in range(GROUP):
            scores = lax.dot_general(
                qs[h], keys, (((1,), (1,)), ((), ())), preferred_element_type=jnp.float32
            )
            pieces = [
                scores[:, c * HEAD_SIZE : (c + 1) * HEAD_SIZE] * SCALE for c in range(parts)
            ]
            if masking:
                pieces = [jnp.where(a, p, MASKED) for a, p in zip(allowed, pieces)]
            top = functools.reduce(jnp.maximum, pieces)
            old = m_ref[h]
            new = jnp.maximum(old, jnp.max(top, axis=1, keepdims=True))
            correction = jnp.exp2(old - new)
            weights = [jnp.exp2(p - new) for p in pieces]
            l_ref[h] = l_ref[h] * correction + functools.reduce(jnp.add, weights)
            rounded = jnp.concatenate([w.astype(jnp.bfloat16) for w in weights], axis=1)
            acc_ref[h] = acc_ref[h] * correction + jnp.dot(
                rounded, values, preferred_element_type=jnp.float32
            )
            m_ref[h] = new

    def loop(begin, end, masking):
        def step(index, carry):
            block(index, masking)
            return carry

        lax.fori_loop(begin, end, step, 0)

    loop(lo, full_lo, True)
    loop(full_lo, full_hi, False)
    loop(full_hi, hi, True)
    for h in range(GROUP):
        total = jnp.sum(l_ref[h], axis=1, keepdims=True)
        out_ref[:, h * HEAD_SIZE : (h + 1) * HEAD_SIZE] = (acc_ref[h] / total).astype(
            jnp.bfloat16
        )


def attend(bounds, queries, key_value, cosine, sine, starts, tile0, tiles, head0):
    count, cols = key_value.shape
    heads = cols // (2 * HEAD_SIZE)
    wide = GROUP * HEAD_SIZE
    grid_spec = pltpu.PrefetchScalarGridSpec(
        num_scalar_prefetch=1,
        grid=(heads, tiles),
        in_specs=[
            pl.BlockSpec((TILE, wide), lambda g, t, s: (t + tile0, g + head0)),
            pl.BlockSpec((count, HEAD_SIZE), lambda g, t, s: (0, g)),
            pl.BlockSpec((count, HEAD_SIZE), lambda g, t, s: (0, g + heads)),
            pl.BlockSpec((TILE, HEAD_SIZE), lambda g, t, s: (t + tile0, 0)),
            pl.BlockSpec((TILE, HEAD_SIZE), lambda g, t, s: (t + tile0, 0)),
            pl.BlockSpec((TILE, HEAD_SIZE), lambda g, t, s: (t + tile0, 0)),
        ],
        out_specs=pl.BlockSpec((TILE, wide), lambda g, t, s: (t, g)),
        scratch_shapes=[
            pltpu.VMEM((GROUP, TILE, HEAD_SIZE), jnp.bfloat16),
            pltpu.VMEM((GROUP, TILE, HEAD_SIZE), jnp.float32),
            pltpu.VMEM((GROUP, TILE, HEAD_SIZE), jnp.float32),
            pltpu.VMEM((GROUP, TILE, HEAD_SIZE), jnp.float32),
        ],
    )
    pairs = heads * GROUP * tiles * TILE * count // 2
    return pl.pallas_call(
        functools.partial(attend_kernel, tile0=tile0),
        grid_spec=grid_spec,
        out_shape=jax.ShapeDtypeStruct((tiles * TILE, heads * wide), jnp.bfloat16),
        compiler_params=pltpu.CompilerParams(
            dimension_semantics=("arbitrary", "arbitrary"), vmem_limit_bytes=40 * 2**20
        ),
        cost_estimate=pl.CostEstimate(
            flops=pairs * HEAD_SIZE * 8,
            bytes_accessed=count * cols * 2,
            transcendentals=pairs,
        ),
    )(bounds, queries, key_value, key_value, cosine, sine, starts)


def shift(array, n_tp, by):
    return lax.ppermute(array, "tp", [(i, (i + by) % n_tp) for i in range(n_tp)])


def gather_features(hidden, n_tp, rank):
    pieces = [hidden] + [shift(hidden, n_tp, by) for by in range(1, n_tp)]
    ordered = []
    for j in range(n_tp):
        which = (rank - j + n_tp) % n_tp
        piece = pieces[0]
        for by in range(1, n_tp):
            piece = jnp.where(which == by, pieces[by], piece)
        ordered.append(piece)
    return jnp.concatenate(ordered, axis=1)


def scatter_features(partial, n_tp, rank):
    width = partial.shape[1] // n_tp
    total = lax.dynamic_slice_in_dim(partial, rank * width, width, 1).astype(jnp.float32)
    for by in range(1, n_tp):
        slab = lax.dynamic_slice_in_dim(partial, (rank + by) % n_tp * width, width, 1)
        total = total + shift(slab, n_tp, by).astype(jnp.float32)
    return total.astype(jnp.bfloat16)


def shards(hidden, norm_gain, w_query, w_key, w_value, w_out, doc_ids, *, n_tp):
    tok_rows = hidden.shape[0]
    width = norm_gain.shape[0]
    local_kv = w_key.shape[1] // HEAD_SIZE
    rank = lax.axis_index("tp")
    cp_rank = lax.axis_index("cp")

    all_docs = lax.all_gather(doc_ids, "cp", axis=0, tiled=True)
    starts = jnp.sum(
        (all_docs[None, :] < doc_ids[:, None]).astype(jnp.int32), axis=1, dtype=jnp.int32
    )
    positions = cp_rank * tok_rows + jnp.arange(tok_rows, dtype=jnp.int32)
    cosine, sine = tables(positions)
    n_tiles = tok_rows // TILE
    first_pos = cp_rank * tok_rows + TILE * jnp.arange(n_tiles, dtype=jnp.int32)
    low = starts[::TILE] // KEYS
    high = (first_pos + TILE + KEYS - 1) // KEYS
    full_low = jnp.clip((starts[TILE - 1 :: TILE] + KEYS - 1) // KEYS, low, high)
    full_high = jnp.clip((first_pos + 1) // KEYS, full_low, high)
    bounds = jnp.stack([low, full_low, full_high, high, first_pos], axis=1)
    starts = jnp.broadcast_to(starts[:, None], (tok_rows, HEAD_SIZE))

    whole = gather_features(hidden, n_tp, rank).astype(jnp.float32)
    inverse_rms = lax.rsqrt(jnp.sum(whole * whole, axis=1) / width + epsilon)[:, None]
    normed = (whole * inverse_rms * norm_gain[None, :]).astype(jnp.bfloat16)

    key_raw = jnp.dot(normed, w_key, preferred_element_type=jnp.float32)
    values = jnp.dot(normed, w_value, preferred_element_type=jnp.float32).astype(jnp.bfloat16)
    key_heads = key_raw.reshape(tok_rows, local_kv, HEAD_SIZE)
    half = HEAD_SIZE // 2
    swapped = jnp.concatenate([key_heads[..., half:], key_heads[..., :half]], axis=-1)
    keys = (
        (key_heads * cosine[:, None, :] + swapped * sine[:, None, :])
        .astype(jnp.bfloat16)
        .reshape(tok_rows, local_kv * HEAD_SIZE)
    )
    cut = local_kv // 2 * HEAD_SIZE
    gathered = []
    for part in (slice(0, cut), slice(cut, None)):
        own = jnp.concatenate([keys[:, part], values[:, part]], axis=1)
        gathered.append(lax.all_gather(own, "cp", axis=0, tiled=True))
    queries = jnp.dot(normed, w_query, preferred_element_type=jnp.float32)

    args = (cosine, sine, starts)
    first = attend(bounds, queries, gathered[0], *args, 0, n_tiles, 0)
    outs = []
    for tile in range(n_tiles):
        second = attend(bounds, queries, gathered[1], *args, tile, 1, local_kv // 2)
        attended = jnp.concatenate([first[tile * TILE : (tile + 1) * TILE], second], axis=1)
        partial = jnp.dot(attended, w_out, preferred_element_type=jnp.float32)
        outs.append(scatter_features(partial.astype(jnp.bfloat16), n_tp, rank))
    return jnp.concatenate(outs, axis=0)


def solution(mesh):
    in_specs = (
        P("cp", "tp"),
        P(),
        P(None, "tp"),
        P(None, "tp"),
        P(None, "tp"),
        P("tp", None),
        P("cp"),
    )
    body = functools.partial(shards, n_tp=mesh.shape["tp"])
    return jax.shard_map(
        body, mesh=mesh, in_specs=in_specs, out_specs=P("cp", "tp"), check_vma=False
    )
```

```python
import functools

import jax
import jax.numpy as jnp
from jax import lax
from jax.experimental import pallas as pl
from jax.experimental.pallas import tpu as pltpu
from jax.sharding import PartitionSpec as P

HEADS = 32
KV_HEADS = 8
HEAD_SIZE = 128
GROUP = HEADS // KV_HEADS

epsilon = 1e-05
rope_base = 500000.0
TILE = 256
KEYS = 512
LOG2E = 1.4426950408889634
SCALE = HEAD_SIZE ** (-0.5) * LOG2E
FLOOR = -1e29
MASKED = -1e30


def tables(positions):
    half = HEAD_SIZE // 2
    freqs = rope_base ** (-jnp.arange(half, dtype=jnp.float32) * 2.0 / HEAD_SIZE)
    angles = positions.astype(jnp.float32)[:, None] * freqs[None, :]
    cosine = jnp.cos(angles)
    sine = jnp.sin(angles)
    return (
        jnp.concatenate([cosine, cosine], axis=1),
        jnp.concatenate([-sine, sine], axis=1),
    )


def attend_kernel(
    bounds, q_ref, k_ref, v_ref, cos_ref, sin_ref, start_ref, out_ref, qs, m_ref, l_ref, acc_ref,
    *, tile0,
):
    tile = pl.program_id(1) + tile0
    lo, full_lo, full_hi, hi, first_pos = (bounds[tile, i] for i in range(5))
    for h in range(GROUP):
        raw = q_ref[:, h * HEAD_SIZE : (h + 1) * HEAD_SIZE]
        turned = raw * cos_ref[...] + pltpu.roll(raw, HEAD_SIZE // 2, 1) * sin_ref[...]
        qs[h] = turned.astype(jnp.bfloat16)
    m_ref[...] = jnp.full_like(m_ref, FLOOR)
    l_ref[...] = jnp.zeros_like(l_ref)
    acc_ref[...] = jnp.zeros_like(acc_ref)
    parts = KEYS // HEAD_SIZE

    def block(index, masking):
        rows = pl.ds(pl.multiple_of(index * KEYS, KEYS), KEYS)
        keys = k_ref[rows, :]
        values = v_ref[rows, :]
        if masking:
            row = lax.broadcasted_iota(jnp.int32, (TILE, HEAD_SIZE), 0)
            lane = lax.broadcasted_iota(jnp.int32, (TILE, HEAD_SIZE), 1)
            last = row + (first_pos - index * KEYS) - lane
            begin = start_ref[...] - index * KEYS - lane
            allowed = [
                (last >= c * HEAD_SIZE) & (begin <= c * HEAD_SIZE) for c in range(parts)
            ]
        for h in range(GROUP):
            scores = lax.dot_general(
                qs[h], keys, (((1,), (1,)), ((), ())), preferred_element_type=jnp.float32
            )
            pieces = [
                scores[:, c * HEAD_SIZE : (c + 1) * HEAD_SIZE] * SCALE for c in range(parts)
            ]
            if masking:
                pieces = [jnp.where(a, p, MASKED) for a, p in zip(allowed, pieces)]
            top = functools.reduce(jnp.maximum, pieces)
            old = m_ref[h]
            new = jnp.maximum(old, jnp.max(top, axis=1, keepdims=True))
            correction = jnp.exp2(old - new)
            weights = [jnp.exp2(p - new) for p in pieces]
            l_ref[h] = l_ref[h] * correction + functools.reduce(jnp.add, weights)
            rounded = jnp.concatenate([w.astype(jnp.bfloat16) for w in weights], axis=1)
            acc_ref[h] = acc_ref[h] * correction + jnp.dot(
                rounded, values, preferred_element_type=jnp.float32
            )
            m_ref[h] = new

    def open_step(index, carry):
        block(index, False)
        return carry

    def edge_step(index, carry):
        block(jnp.where(index < full_lo, index, index + (full_hi - full_lo)), True)
        return carry

    lax.fori_loop(full_lo, full_hi, open_step, 0)
    lax.fori_loop(lo, hi - (full_hi - full_lo), edge_step, 0)
    for h in range(GROUP):
        total = jnp.sum(l_ref[h], axis=1, keepdims=True)
        out_ref[:, h * HEAD_SIZE : (h + 1) * HEAD_SIZE] = (acc_ref[h] / total).astype(
            jnp.bfloat16
        )


def key_value_kernel(key_ref, value_ref, cos_ref, sin_ref, *outs):
    for h, out_ref in enumerate(outs):
        cols = slice(h * HEAD_SIZE, (h + 1) * HEAD_SIZE)
        raw = key_ref[:, cols]
        turned = raw * cos_ref[...] + pltpu.roll(raw, HEAD_SIZE // 2, 1) * sin_ref[...]
        out_ref[:, :HEAD_SIZE] = turned.astype(jnp.bfloat16)
        out_ref[:, HEAD_SIZE:] = value_ref[:, cols].astype(jnp.bfloat16)


def key_value_heads(key_raw, value_raw, cosine, sine):
    rows, cols = key_raw.shape
    shape = jax.ShapeDtypeStruct((rows, 2 * HEAD_SIZE), jnp.bfloat16)
    return pl.pallas_call(key_value_kernel, out_shape=[shape] * (cols // HEAD_SIZE))(
        key_raw, value_raw, cosine, sine
    )


def attend(bounds, queries, key_value, cosine, sine, starts, tile0, tiles, head0):
    count, cols = key_value.shape
    heads = cols // (2 * HEAD_SIZE)
    wide = GROUP * HEAD_SIZE
    grid_spec = pltpu.PrefetchScalarGridSpec(
        num_scalar_prefetch=1,
        grid=(heads, tiles),
        in_specs=[
            pl.BlockSpec((TILE, wide), lambda g, t, s: (t + tile0, g + head0)),
            pl.BlockSpec((count, HEAD_SIZE), lambda g, t, s: (0, g)),
            pl.BlockSpec((count, HEAD_SIZE), lambda g, t, s: (0, g + heads)),
            pl.BlockSpec((TILE, HEAD_SIZE), lambda g, t, s: (t + tile0, 0)),
            pl.BlockSpec((TILE, HEAD_SIZE), lambda g, t, s: (t + tile0, 0)),
            pl.BlockSpec((TILE, HEAD_SIZE), lambda g, t, s: (t + tile0, 0)),
        ],
        out_specs=pl.BlockSpec((TILE, wide), lambda g, t, s: (t, g)),
        scratch_shapes=[
            pltpu.VMEM((GROUP, TILE, HEAD_SIZE), jnp.bfloat16),
            pltpu.VMEM((GROUP, TILE, HEAD_SIZE), jnp.float32),
            pltpu.VMEM((GROUP, TILE, HEAD_SIZE), jnp.float32),
            pltpu.VMEM((GROUP, TILE, HEAD_SIZE), jnp.float32),
        ],
    )
    pairs = heads * GROUP * tiles * TILE * count // 2
    return pl.pallas_call(
        functools.partial(attend_kernel, tile0=tile0),
        grid_spec=grid_spec,
        out_shape=jax.ShapeDtypeStruct((tiles * TILE, heads * wide), jnp.bfloat16),
        compiler_params=pltpu.CompilerParams(
            dimension_semantics=("arbitrary", "arbitrary"), vmem_limit_bytes=60 * 2**20
        ),
        cost_estimate=pl.CostEstimate(
            flops=pairs * HEAD_SIZE * 8,
            bytes_accessed=count * cols * 2,
            transcendentals=pairs,
        ),
    )(bounds, queries, key_value, key_value, cosine, sine, starts)


def shift(array, n_tp, by):
    return lax.ppermute(array, "tp", [(i, (i + by) % n_tp) for i in range(n_tp)])


def gather_features(hidden, n_tp, rank):
    pieces = [hidden] + [shift(hidden, n_tp, by) for by in range(1, n_tp)]
    ordered = []
    for j in range(n_tp):
        which = (rank - j + n_tp) % n_tp
        piece = pieces[0]
        for by in range(1, n_tp):
            piece = jnp.where(which == by, pieces[by], piece)
        ordered.append(piece)
    return jnp.concatenate(ordered, axis=1)


def scatter_features(partial, n_tp, rank):
    width = partial.shape[1] // n_tp
    total = lax.dynamic_slice_in_dim(partial, rank * width, width, 1).astype(jnp.float32)
    for by in range(1, n_tp):
        slab = lax.dynamic_slice_in_dim(partial, (rank + by) % n_tp * width, width, 1)
        total = total + shift(slab, n_tp, by).astype(jnp.float32)
    return total.astype(jnp.bfloat16)


def shards(hidden, norm_gain, w_query, w_key, w_value, w_out, doc_ids, *, n_tp):
    tok_rows = hidden.shape[0]
    width = norm_gain.shape[0]
    local_kv = w_key.shape[1] // HEAD_SIZE
    rank = lax.axis_index("tp")
    cp_rank = lax.axis_index("cp")

    all_docs = lax.all_gather(doc_ids, "cp", axis=0, tiled=True)
    starts = jnp.sum(
        (all_docs[None, :] < doc_ids[:, None]).astype(jnp.int32), axis=1, dtype=jnp.int32
    )
    positions = cp_rank * tok_rows + jnp.arange(tok_rows, dtype=jnp.int32)
    cosine, sine = tables(positions)
    n_tiles = tok_rows // TILE
    first_pos = cp_rank * tok_rows + TILE * jnp.arange(n_tiles, dtype=jnp.int32)
    low = starts[::TILE] // KEYS
    high = (first_pos + TILE + KEYS - 1) // KEYS
    full_low = jnp.clip((starts[TILE - 1 :: TILE] + KEYS - 1) // KEYS, low, high)
    full_high = jnp.clip((first_pos + 1) // KEYS, full_low, high)
    bounds = jnp.stack([low, full_low, full_high, high, first_pos], axis=1)
    starts = jnp.broadcast_to(starts[:, None], (tok_rows, HEAD_SIZE))

    whole = gather_features(hidden, n_tp, rank).astype(jnp.float32)
    inverse_rms = lax.rsqrt(jnp.sum(whole * whole, axis=1) / width + epsilon)[:, None]
    normed = (whole * inverse_rms * norm_gain[None, :]).astype(jnp.bfloat16)

    key_raw = jnp.dot(normed, w_key, preferred_element_type=jnp.float32)
    value_raw = jnp.dot(normed, w_value, preferred_element_type=jnp.float32)
    gathered = [
        lax.all_gather(own, "cp", axis=0, tiled=True)
        for own in key_value_heads(key_raw, value_raw, cosine, sine)
    ]
    queries = jnp.dot(normed, w_query, preferred_element_type=jnp.float32)

    args = (cosine, sine, starts)
    first = [
        attend(bounds, queries, gathered[g], *args, 0, n_tiles, g) for g in range(local_kv - 1)
    ]
    outs = []
    for tile in range(n_tiles):
        last = attend(bounds, queries, gathered[-1], *args, tile, 1, local_kv - 1)
        rows = slice(tile * TILE, (tile + 1) * TILE)
        attended = jnp.concatenate([part[rows] for part in first] + [last], axis=1)
        partial = jnp.dot(attended, w_out, preferred_element_type=jnp.float32)
        outs.append(scatter_features(partial.astype(jnp.bfloat16), n_tp, rank))
    return jnp.concatenate(outs, axis=0)


def solution(mesh):
    in_specs = (
        P("cp", "tp"),
        P(),
        P(None, "tp"),
        P(None, "tp"),
        P(None, "tp"),
        P("tp", None),
        P("cp"),
    )
    body = functools.partial(shards, n_tp=mesh.shape["tp"])
    return jax.shard_map(
        body, mesh=mesh, in_specs=in_specs, out_specs=P("cp", "tp"), check_vma=False
    )
```
